32 devices in a mesh: kpt: 4 (over y, x), grid: 8 (over z, core).
Axes of the slice: x: 2, y: 2, z: 4, core: 2. Of those that a mesh axis runs over, the one named last changes fastest.
Arguments:
- bands: float32 [4, 2, 2, 48, 2304], P('kpt', None, None, 'grid'), may hold values from -6 to 6
- potential: float32 [48, 2304], P('grid'), may hold values from -4 to 4
- phase_numerator_table: int32 [4, 3], P('kpt'), may hold values from 0 to 7
- kweight: float32 [4], P('kpt'), may hold values from 0.25 to 2
- lowest: float32 [4], P('kpt'), may hold values from -6 to -4.5
- cut: float32 [4], P('kpt'), may hold values from 0 to 3
- upper: float32 [4], P('kpt'), may hold values from 15 to 17
- fermi: float32 [1], replicated, may hold values from -0.5 to 1.5
Outputs:
- filtered: float32 [4, 2, 2, 48, 2304], P('kpt', None, None, 'grid')
- band_energies: float32 [4, 2], P('kpt')
- total_energy: float32 [1], replicated
The draws below stay inside these ranges and needn't reach their ends.
All inputs are finite; a program needn't handle non-finite values.
Results may differ from the reference program's by a relative error of at most 0.00022.
Values sent between devices are 32-bit elements; how exact they have to be, the bound alone decides.
A program may use at most 128 MiB of HBM per device.

```python
import math
import jax
import jax.numpy as jnp
from jax import lax

BAND_TOTAL = 2
CELLS_SECOND = 48
CELLS_THIRD = 48
DEGREE = 6
PHASE_DIVISOR = 8
KPOINT_TOTAL = 4
CELLS_FIRST = 48


def plant(drawn, rng, low, high):
    place = [jax.random.randint(jax.random.fold_in(rng, axis), (), 0, length) for axis, length in enumerate(drawn.shape)]
    longest = drawn.shape.index(max(drawn.shape))
    neighbour = place[:longest] + [(place[longest] + 1) % drawn.shape[longest]] + place[longest + 1:]
    return drawn.at[tuple(place)].set(low).at[tuple(neighbour)].set(high)


def levels(key, extent, cuts, low, largest):
    factor_of = 1.0
    for position, shards_of in cuts:
        heights = jax.random.uniform(jax.random.fold_in(jax.random.fold_in(key, 6), position), (shards_of,), jnp.float32, low / len(cuts), largest / len(cuts))
        factor_of = factor_of * jnp.repeat(jnp.exp(heights), extent[position] // shards_of).reshape((-1,) + (1,) * (len(extent) - 1 - position))
    return factor_of


def gaussian(rng, dims, width, most, split=(), kind=jnp.bfloat16):
    values = jax.random.normal(rng, dims, jnp.float32) * width
    if len(split) > 0:
        values = levels(rng, dims, split, -0.22, 0.18) * values
    return jnp.clip(values, min=-most, max=most).astype(kind)


def setup_inputs(seed: int = 0) -> dict:
    streams_of = jax.random.split(jax.random.key(seed), 9)
    bands = gaussian(streams_of[0], (KPOINT_TOTAL, 2, BAND_TOTAL, CELLS_FIRST, CELLS_SECOND * CELLS_THIRD), 1.0, 6.0, ((0, 4), (3, 8)), jnp.float32)
    potential = gaussian(streams_of[1], (CELLS_FIRST, CELLS_SECOND * CELLS_THIRD), 1.0, 4.0, ((0, 8),), jnp.float32)
    phase_numerator_table = plant(jax.random.randint(streams_of[2], (KPOINT_TOTAL, 3), 0, PHASE_DIVISOR), jax.random.fold_in(streams_of[2], 1), 0, PHASE_DIVISOR - 1).astype(jnp.int32)
    kweight = jnp.clip(jnp.exp(math.log(2.0) - 2.0794415 * jax.random.uniform(streams_of[3], (KPOINT_TOTAL,), jnp.float32) ** levels(streams_of[3], (KPOINT_TOTAL,), ((0, 4),), -0.2, 0.2)), 0.25, 2.0)
    lowest = jnp.clip(-6.0 + 1.5 * jax.random.uniform(streams_of[4], (KPOINT_TOTAL,), jnp.float32) ** levels(streams_of[4], (KPOINT_TOTAL,), ((0, 4),), -0.2, 0.2), -6.0, -4.5)
    cut = jnp.clip(3.0 * jax.random.uniform(streams_of[5], (KPOINT_TOTAL,), jnp.float32) ** levels(streams_of[5], (KPOINT_TOTAL,), ((0, 4),), -0.2, 0.2), 0.0, 3.0)
    upper = jnp.clip(15.0 + 2.0 * jax.random.uniform(streams_of[6], (KPOINT_TOTAL,), jnp.float32) ** levels(streams_of[6], (KPOINT_TOTAL,), ((0, 4),), -0.2, 0.2), 15.0, 17.0)
    fermi = jnp.clip(jax.random.uniform(streams_of[7], (1,), jnp.float32, -0.5, 1.5), -0.5, 1.5)
    return dict(bands=bands, potential=potential, phase_numerator_table=phase_numerator_table, kweight=kweight, lowest=lowest, cut=cut, upper=upper, fermi=fermi)


coefficients = (-5369.0 / 1800.0, 12.0 / 7.0, -15.0 / 56.0, 10.0 / 189.0, -1.0 / 112.0, 2.0 / 1925.0, -1.0 / 16632.0)
smearing = 0.5


def twist(part, angle):
    cosine = jnp.cos(angle)
    sine = jnp.sin(angle)
    return jnp.stack([part[0] * cosine - part[1] * sine, part[0] * sine + part[1] * cosine])


def second_diff(extended, axis, length):
    reach = len(coefficients) - 1
    filter_result = coefficients[0] * lax.slice_in_dim(extended, reach, reach + length, axis=axis)
    for offset in range(1, reach + 1):
        upward = lax.slice_in_dim(extended, reach + offset, reach + offset + length, axis=axis)
        downward = lax.slice_in_dim(extended, reach - offset, reach - offset + length, axis=axis)
        filter_result = filter_result + coefficients[offset] * (upward + downward)
    return filter_result


def extend_local(wave_field, axis, angle):
    reach = len(coefficients) - 1
    length = wave_field.shape[axis]
    lower = twist(lax.slice_in_dim(wave_field, length - reach, length, axis=axis), -angle)
    higher = twist(lax.slice_in_dim(wave_field, 0, reach, axis=axis), angle)
    return jnp.concatenate([lower, wave_field, higher], axis=axis)


def apply_h(wave_field, potential, bloch_angles):
    laplace = second_diff(extend_local(wave_field, 2, bloch_angles[0]), 2, wave_field.shape[2])
    laplace = laplace + second_diff(extend_local(wave_field, 3, bloch_angles[1]), 3, wave_field.shape[3])
    laplace = laplace + second_diff(extend_local(wave_field, 4, bloch_angles[2]), 4, wave_field.shape[4])
    return -0.5 * laplace + potential * wave_field


def chebyshev_filter(wave_field, hamiltonian_operator, low_end, cut_end, high_end):
    half_width = (high_end - cut_end) / 2.0
    centre = (high_end + cut_end) / 2.0
    first_sigma = half_width / (low_end - centre)
    sigma = first_sigma
    previous = wave_field
    current = (hamiltonian_operator(wave_field) - centre * wave_field) * (first_sigma / half_width)
    for degree in range(1, DEGREE):
        next_sigma = 1.0 / (2.0 / first_sigma - sigma)
        following = (hamiltonian_operator(current) - centre * current) * (2.0 * next_sigma / half_width) - (sigma * next_sigma) * previous
        previous = current
        current = following
        sigma = next_sigma
    return current


def reference(bands, potential, phase_numerator_table, kweight, lowest, cut, upper, fermi):
    grid_potential = potential.reshape(CELLS_FIRST, CELLS_SECOND, CELLS_THIRD)
    outputs = []
    energies = []
    energy_grand_sum = jnp.zeros((1,), jnp.float32)
    for kpoint_index in range(KPOINT_TOTAL):
        wave_field = bands[kpoint_index].reshape(2, BAND_TOTAL, CELLS_FIRST, CELLS_SECOND, CELLS_THIRD)
        bloch_angles = 2.0 * jnp.pi * phase_numerator_table[kpoint_index].astype(jnp.float32) / PHASE_DIVISOR

        def hamiltonian_operator(value):
            return apply_h(value, grid_potential, bloch_angles)

        filter_result = chebyshev_filter(wave_field, hamiltonian_operator, lowest[kpoint_index], cut[kpoint_index], upper[kpoint_index])
        applied = hamiltonian_operator(filter_result)
        numerator = jnp.sum(filter_result * applied, axis=(0, 2, 3, 4))
        denominator = jnp.sum(filter_result * filter_result, axis=(0, 2, 3, 4))
        band_energy = numerator / denominator
        band_occupation = 1.0 / (1.0 + jnp.exp((band_energy - fermi[0]) / smearing))
        energy_grand_sum = energy_grand_sum + kweight[kpoint_index] * jnp.sum(band_occupation * band_energy)
        outputs.append(filter_result.reshape(2, BAND_TOTAL, CELLS_FIRST, CELLS_SECOND * CELLS_THIRD))
        energies.append(band_energy)
    return jnp.stack(outputs), jnp.stack(energies), energy_grand_sum
```

```python
import functools

import jax
import jax.numpy as jnp
import numpy as np
from jax import lax
from jax.experimental import pallas as pl
from jax.experimental.layout import Layout, with_layout_constraint
from jax.experimental.pallas import tpu as pltpu
from jax.sharding import PartitionSpec as P

SIDE = 48
DEGREE = 6
PHASE_DIVISOR = 8
REACH = 6
LANES = 128
USED = 2 * SIDE
PAD = 8
ROWS = SIDE + 2 * PAD
TILES = SIDE // 8
CHUNKS = SIDE * SIDE // LANES
PER_TILE = CHUNKS // TILES
BANDS = 2

coefficients = (
    -5369.0 / 1800.0,
    12.0 / 7.0,
    -15.0 / 56.0,
    10.0 / 189.0,
    -1.0 / 112.0,
    2.0 / 1925.0,
    -1.0 / 16632.0,
)
smearing = 0.5
MESH = pl.DeviceIdType.MESH


def third_parts():
    inside = np.zeros((SIDE, SIDE))
    over = np.zeros((SIDE, SIDE))
    under = np.zeros((SIDE, SIDE))
    for z in range(SIDE):
        for j in range(1, REACH + 1):
            weight = -0.5 * coefficients[j]
            for target, sign in ((z + j, 1), (z - j, -1)):
                if 0 <= target < SIDE:
                    inside[target, z] += weight
                elif sign > 0:
                    over[target - SIDE, z] += weight
                else:
                    under[target + SIDE, z] += weight
    plain = np.zeros((LANES, LANES))
    cosine = np.zeros((LANES, LANES))
    sine = np.zeros((LANES, LANES))
    both, apart = over + under, over - under
    for c in range(2):
        s = slice(c * SIDE, (c + 1) * SIDE)
        plain[s, s] = inside
        cosine[s, s] = both
    re, im = slice(0, SIDE), slice(SIDE, USED)
    sine[im, re] = -apart
    sine[re, im] = apart
    return [a.astype(np.float32) for a in (plain, cosine, sine)]


def kernel(
    n,
    members_k,
    planes,
    table_hbm,
    kweight_hbm,
    lowest_hbm,
    cut_hbm,
    upper_hbm,
    fermi_hbm,
    bands_hbm,
    pot_hbm,
    parts_hbm,
    out_ref,
    energy_ref,
    total_ref,
    table_ref,
    kweight_ref,
    lowest_ref,
    cut_ref,
    upper_ref,
    fermi_ref,
    own,
    own_pot,
    parts_ref,
    field_0,
    field_1,
    field_2,
    mat_ref,
    potential,
    stage,
    stage_pot,
    turned,
    rolled,
    packed,
    part,
    part_k,
    load_sem,
    send,
    recv,
    send_pot,
    recv_pot,
    halo_send,
    halo_recv,
    out_send,
    out_recv,
    send_red,
    recv_red,
    send_k,
    recv_k,
):
    fields = (field_0, field_1, field_2)
    chips = n // 2
    slabs = n // 2
    total_planes = slabs * planes
    first_worker = 2 * (chips // 2 - 1)
    workers = 2 * BANDS
    me = lax.axis_index("grid")
    kpt = lax.axis_index("kpt")
    core = lax.rem(me, 2)
    partner = me + 1 - 2 * core
    is_worker = (me >= first_worker) & (me < first_worker + workers)
    my_band = lax.div(me - first_worker, 2)
    my_half = lax.div(me, slabs)
    my_slot = lax.rem(me, slabs)

    loads = [
        pltpu.make_async_copy(src, dst, load_sem.at[i])
        for i, (src, dst) in enumerate(
            (
                (table_hbm, table_ref),
                (kweight_hbm, kweight_ref),
                (lowest_hbm, lowest_ref),
                (cut_hbm, cut_ref),
                (upper_hbm, upper_ref),
                (fermi_hbm, fermi_ref),
                (parts_hbm, parts_ref),
                (pot_hbm, own_pot),
                (bands_hbm.at[:, 0], own.at[0]),
                (bands_hbm.at[:, 1], own.at[1]),
            )
        )
    ]
    for load in loads[::-1]:
        load.start()

    barrier = pltpu.get_barrier_semaphore()

    def greet(target_k, target):
        pl.semaphore_signal(barrier, inc=1, device_id=(target_k, target), device_id_type=MESH)

    for d in range(1, members_k):
        greet(lax.rem(kpt + d, members_k), me)

    @pl.when(is_worker)
    def _():
        for d in range(1, n):
            greet(kpt, lax.rem(me + d, n))

    @pl.when(jnp.logical_not(is_worker))
    def _():
        for w in range(workers):
            greet(kpt, first_worker + w)

    loads[7].wait()
    loads[8].wait()
    loads[9].wait()
    pl.semaphore_wait(
        barrier, jnp.where(is_worker, n - 1 + members_k - 1, workers + members_k - 1)
    )

    def remote(src, dst, ssem, rsem, target):
        return pltpu.make_async_remote_copy(
            src_ref=src,
            dst_ref=dst,
            send_sem=ssem,
            recv_sem=rsem,
            device_id=(kpt, target),
            device_id_type=MESH,
        )

    def deliver(i):
        b = 1 - my_half if i == 0 else my_half
        target = first_worker + 2 * b + my_half
        wave = remote(own.at[b], stage.at[my_slot], send.at[i], recv.at[my_slot], target)
        pot = remote(own_pot, stage_pot.at[my_slot], send_pot.at[i], recv_pot.at[my_slot], target)
        return wave, pot, target

    for i in range(BANDS):
        wave, pot, target = deliver(i)

        @pl.when(target != me)
        def _():
            wave.start()
            pot.start()

    lane = lax.broadcasted_iota(jnp.int32, (8, LANES), 1)
    row = lax.broadcasted_iota(jnp.int32, (8, LANES), 0)
    first = lane < SIDE
    used = lane < USED
    zero = jnp.zeros((8, LANES), jnp.float32)

    def turn(v, cosine, sine):
        other = jnp.where(first, pltpu.roll(v, LANES - SIDE, 1), pltpu.roll(v, SIDE, 1))
        signed = jnp.where(used, jnp.where(first, -sine, sine), 0.0)
        return cosine * v + signed * other

    def spread(scalar):
        return jnp.full((8, LANES), scalar)

    for i in range(7):
        loads[i].wait()

    low_end, cut_end, high_end = (spread(r[0]) for r in (lowest_ref, cut_ref, upper_ref))
    half_width = (high_end - cut_end) / 2.0
    centre = (high_end + cut_end) / 2.0

    @pl.when(is_worker)
    def _():
        def phase(d):
            numerator = spread(table_ref[0, d])
            cosine, sine = jnp.ones((8, LANES), jnp.float32), zero
            for i in range(1, PHASE_DIVISOR):
                here = numerator == i
                angle = 2.0 * np.pi * i / PHASE_DIVISOR
                cosine = jnp.where(here, float(np.cos(angle)), cosine)
                sine = jnp.where(here, float(np.sin(angle)), sine)
            return cosine, sine

        cos_x, sin_x = phase(0)
        cos_y, sin_y = phase(1)
        cos_z, sin_z = phase(2)
        at_low = spread(core) == 0
        side_turn = (
            (jnp.where(at_low, cos_x, 1.0), jnp.where(at_low, sin_x, 0.0)),
            (jnp.where(at_low, 1.0, cos_x), jnp.where(at_low, 0.0, -sin_x)),
        )
        first_sigma = half_width / (low_end - centre)
        sigma = first_sigma
        final_scale = first_sigma
        for degree in range(1, DEGREE):
            sigma = 1.0 / (2.0 / first_sigma - sigma)
            final_scale = final_scale * sigma
        scale = 2.0 / half_width
        weights = [scale * (-0.5 * c) for c in coefficients]

        for r in range(LANES // 16):
            rows = pl.ds(16 * r, 16)
            cosine = jnp.concatenate([cos_z, cos_z], axis=0)
            sine = jnp.concatenate([sin_z, sin_z], axis=0)
            entry = (
                parts_ref[0, rows, :] + cosine * parts_ref[1, rows, :] + sine * parts_ref[2, rows, :]
            )
            entry = entry * jnp.concatenate([scale, scale], axis=0)
            high = entry.astype(jnp.bfloat16)
            rest = (entry - high.astype(jnp.float32)).astype(jnp.bfloat16)
            lower = pl.ds(LANES + 16 * r, 16)
            mat_ref[rows, pl.ds(0, LANES)] = high
            mat_ref[rows, pl.ds(LANES, LANES)] = rest
            mat_ref[lower, pl.ds(0, LANES)] = high
            mat_ref[lower, pl.ds(LANES, LANES)] = jnp.zeros_like(high)

        def clear(p, carry):
            for t in range(TILES):
                field_2[planes + p, pl.ds(PAD + 8 * t, 8), :] = zero
            return carry

        lax.fori_loop(0, total_planes, clear, 0)

        def put(f, plane, t, v):
            f[plane, pl.ds(PAD + 8 * t, 8), :] = v
            if t == 0:
                f[plane, pl.ds(PAD + SIDE, 8), :] = turn(v, cos_y, sin_y)
            if t == TILES - 1:
                f[plane, pl.ds(0, 8), :] = turn(v, cos_y, -sin_y)

        def ordering(part_index):
            begin = SIDE * lax.rem(5 * row + part_index, 8)
            which = lax.shift_right_logical(begin + ((lane - begin) & (LANES - 1)), 7)
            return which, lax.rem(5 * row + 3 * part_index, 8)

        orders = [ordering(i) for i in range(2)]

        def lay(load, part_index):
            which, back = orders[part_index]
            ahead = [jnp.broadcast_to(load(i), (8, LANES)) for i in range(PER_TILE)]
            v = jnp.where(which == 0, ahead[0], jnp.where(which == 1, ahead[1], ahead[2]))
            v = pltpu.roll(v, 0, 1, stride=16, stride_axis=0)
            return jnp.take_along_axis(v, back, axis=0)

        flat = stage.reshape(slabs, 2 * planes * CHUNKS, LANES)

        def unpack(slot):
            for p in range(planes):
                for t in range(TILES):
                    def rows_of(part_index):
                        base = (part_index * planes + p) * CHUNKS + PER_TILE * t
                        return lay(
                            lambda i: flat[slot, pl.ds(base + i, 1), :], part_index
                        )

                    v = jnp.where(first, rows_of(0), jnp.where(used, rows_of(1), 0.0))
                    put(field_0, planes + slot * planes + p, t, v)

        def unpack_pot(slot):
            for p in range(planes):
                for t in range(TILES):
                    v = lay(
                        lambda i: stage_pot[
                            slot, pl.ds(p, 1), pl.ds((PER_TILE * t + i) * LANES, LANES)
                        ],
                        0,
                    )
                    v = (v - 1.5 * coefficients[0] - centre) * scale
                    v = jnp.where(first, v, jnp.where(used, pltpu.roll(v, SIDE, 1), 0.0))
                    potential[slot * planes + p, pl.ds(8 * t, 8), :] = v

        def take(i, carry):
            slot = jnp.where(core == 0, slabs - 1 - i, i)

            @pl.when(half_base + slot != me)
            def _():
                remote(stage.at[slot], stage.at[slot], send.at[0], recv.at[slot], partner).wait_recv()
                remote(
                    stage_pot.at[slot], stage_pot.at[slot], send_pot.at[0], recv_pot.at[slot], partner
                ).wait_recv()

            unpack(slot)
            unpack_pot(slot)
            return carry

        half_base = core * slabs

        @pl.when(my_half == core)
        def _():
            own_flat = own.reshape(BANDS, 2 * planes * CHUNKS, LANES)
            for r in range(2 * planes * CHUNKS // 8):
                flat[my_slot, pl.ds(8 * r, 8), :] = own_flat[my_band, pl.ds(8 * r, 8), :]
            for c in range(CHUNKS):
                part_of = pl.ds(c * LANES, LANES)
                stage_pot[my_slot, :, part_of] = own_pot[:, part_of]

        lax.fori_loop(0, slabs, take, 0)

        body = pl.ds(PAD, SIDE)

        def halo(f, side, parity):
            there = total_planes + planes if side == 0 else 0
            return remote(
                turned.at[side],
                f.at[pl.ds(there, planes), body, :],
                halo_send.at[side],
                halo_recv.at[1 - side, parity],
                partner,
            )

        def hold(side, p, t, v):
            turned[side, p, pl.ds(8 * t, 8), :] = turn(v, *side_turn[side])

        for side in range(2):
            base = planes if side == 0 else total_planes

            for p in range(planes):
                for t in range(TILES):
                    hold(side, p, t, field_0[base + p, pl.ds(PAD + 8 * t, 8), :])
            halo(field_0, side, 0).start()

        def apply(f, k):
            base = k * planes
            middle = [f[base + planes + p, body, :] for p in range(planes)]
            rows = jnp.concatenate(middle, axis=0)
            high = rows.astype(jnp.bfloat16)
            rest = (rows - high.astype(jnp.float32)).astype(jnp.bfloat16)
            both = jnp.concatenate([high, rest], axis=1)
            third = jnp.dot(both, mat_ref[...], preferred_element_type=jnp.float32)
            third = third[:, :LANES] + third[:, LANES:]
            for t in range(TILES):
                tile = pl.ds(PAD + 8 * t, 8)
                window = [f[base + i, tile, :] for i in range(3 * planes)]
                for p in range(planes):
                    value = window[planes + p]
                    total = third[p * SIDE + 8 * t : p * SIDE + 8 * t + 8, :]
                    total = total + value * potential[base + p, pl.ds(8 * t, 8), :]
                    for j in range(1, REACH + 1):
                        around = window[planes + p + j] + window[planes + p - j]
                        above = f[base + planes + p, pl.ds(PAD + 8 * t + j, 8), :]
                        below = f[base + planes + p, pl.ds(PAD + 8 * t - j, 8), :]
                        total = total + weights[j] * (around + (above + below))
                    yield p, base + planes + p, t, tile, value, total

        def await_halos(f, parity):
            for side in range(2):
                halo(f, side, parity).wait_send()
            for side in range(2):
                there = total_planes + planes if side == 1 else 0
                landed = f.at[pl.ds(there, planes), body, :]
                remote(
                    landed, landed, halo_send.at[side], halo_recv.at[side, parity], partner
                ).wait_recv()

        def step(m, c):
            now, then, before = (fields[(c + i) % 3] for i in range(3))
            gain = jnp.where(m == 1, 0.5, 1.0)

            def block(k, side=None):
                for p, plane, t, tile, _, total in apply(now, k):
                    following = gain * total - before[plane, tile, :]
                    put(then, plane, t, following)
                    if side is not None:
                        hold(side, p, t, following)

            def inner(k, carry):
                block(k)
                return carry

            lax.fori_loop(1, slabs - 1, inner, 0)
            parity = lax.rem(m - 1, 2)
            await_halos(now, parity)
            block(0, 0)
            halo(then, 0, 1 - parity).start()
            block(slabs - 1, 1)
            halo(then, 1, 1 - parity).start()

        def three(r, carry):
            for c in range(3):
                step(3 * r + c + 1, c)
            return carry

        lax.fori_loop(0, DEGREE // 3, three, 0)
        final = field_0

        flat_packed = packed.reshape(slabs, 2 * planes * CHUNKS, LANES)
        gather_rows = [lax.rem(3 * row + i, 8) for i in range(2)]
        lane6 = lax.broadcasted_iota(jnp.int32, (TILES, LANES), 1)

        def give(slot):
            return remote(
                packed.at[slot],
                out_ref.at[:, my_band],
                out_send.at[slot],
                out_recv.at[my_band],
                core * slabs + slot,
            )

        def give_here(slot):
            return pltpu.make_async_copy(
                packed.at[slot], out_ref.at[:, my_band], out_recv.at[my_band]
            )

        def pack(i, carry):
            slot = jnp.where(core == 0, i, slabs - 1 - i)

            for p in range(planes):
                plane = planes + slot * planes + p
                for part_index in range(2):
                    lot = 2 * p + part_index
                    for t in range(TILES):
                        v = final[plane, pl.ds(PAD + 8 * t, 8), :] * final_scale
                        v = jnp.take_along_axis(v, gather_rows[part_index], axis=0)
                        v = pltpu.roll(v, 0, 1, stride=16, stride_axis=0)
                        rolled[lot, pl.ds(8 * t, 8), :] = v
            for p in range(planes):
                for part_index in range(2):
                    lot = 2 * p + part_index
                    picks = [
                        rolled[lot, pl.ds((3 * i + 5 * part_index) % 8, TILES, stride=8), :]
                        for i in range(8)
                    ]

                    def choose(*ends):
                        start = ends[0]
                        v = picks[start + len(ends) - 1]
                        for i in range(len(ends) - 2, -1, -1):
                            v = jnp.where(lane6 < ends[i + 1], picks[start + i], v)
                        return v

                    rows = (choose(0, 48, 96), choose(2, 16, 64, 112), choose(5, 32, 80))
                    base = (part_index * planes + p) * CHUNKS
                    for j in range(PER_TILE):
                        flat_packed[slot, pl.ds(base + j, TILES, stride=PER_TILE), :] = rows[j]

            @pl.when(core * slabs + slot != me)
            def _():
                give(slot).start()

            @pl.when(core * slabs + slot == me)
            def _():
                give_here(slot).start()

            return carry

        lax.fori_loop(0, slabs, pack, 0)

        def sums(k, carry):
            tops, bottoms = list(carry[0]), list(carry[1])
            for _, _, t, _, value, total in apply(final, k):
                tops[t % 2] = tops[t % 2] + value * total
                bottoms[t % 2] = bottoms[t % 2] + value * value
            return tuple(tops), tuple(bottoms)

        carry = ((zero, zero), (zero, zero))
        carry = lax.fori_loop(1, slabs - 1, sums, carry)
        await_halos(final, DEGREE % 2)
        carry = sums(0, carry)
        tops, bottoms = sums(slabs - 1, carry)
        top = jnp.sum(tops[0] + tops[1], keepdims=True)
        bottom = jnp.sum(bottoms[0] + bottoms[1], keepdims=True)
        left = lax.broadcasted_iota(jnp.int32, (1, LANES), 1) < LANES // 2
        part[me - first_worker] = jnp.where(left, top, bottom)
        for d in range(1, n):
            remote(
                part.at[me - first_worker],
                part.at[me - first_worker],
                send_red.at[d],
                recv_red.at[me - first_worker],
                lax.rem(me + d, n),
            ).start()

    for w in range(workers):

        @pl.when(me != first_worker + w)
        def _():
            remote(part.at[w], part.at[w], send_red.at[0], recv_red.at[w], first_worker + w).wait_recv()

    kweight, fermi = kweight_ref[0], fermi_ref[0]
    e_half, c_half = half_width[0:1, :], centre[0:1, :]
    term = jnp.zeros((1, LANES), jnp.float32)
    for b in range(BANDS):
        both = part[2 * b] + part[2 * b + 1]
        energy = (0.5 * e_half) * (both / pltpu.roll(both, LANES // 2, 1)) + c_half
        energy_ref[0, b] = energy[0, 0]
        term = term + energy / (1.0 + jnp.exp((energy - fermi) / smearing))
    part_k[kpt] = kweight * term

    def across(d, source, target):
        return pltpu.make_async_remote_copy(
            src_ref=part_k.at[source],
            dst_ref=part_k.at[source],
            send_sem=send_k.at[d],
            recv_sem=recv_k.at[source],
            device_id=(target, me),
            device_id_type=MESH,
        )

    for d in range(1, members_k):
        across(d, kpt, lax.rem(kpt + d, members_k)).start()
    for d in range(1, members_k):
        source = lax.rem(kpt + d, members_k)
        across(d, source, source).wait_recv()
    grand = jnp.zeros((1, LANES), jnp.float32)
    for k in range(members_k):
        grand = grand + part_k[k]
    total_ref[0, 0] = grand[0, 0]

    for b in range(BANDS):
        landing = out_ref.at[:, b]
        remote(landing, landing, out_send.at[0], out_recv.at[b], partner).wait_recv()

    for i in range(BANDS):
        wave, pot, target = deliver(i)

        @pl.when(target != me)
        def _():
            wave.wait_send()
            pot.wait_send()

    for d in range(1, members_k):
        across(d, kpt, lax.rem(kpt + d, members_k)).wait_send()

    @pl.when(is_worker)
    def _():
        for d in range(1, n):
            remote(
                part.at[me - first_worker],
                part.at[me - first_worker],
                send_red.at[d],
                recv_red.at[me - first_worker],
                lax.rem(me + d, n),
            ).wait_send()

        def drain(slot, carry):
            @pl.when(core * slabs + slot != me)
            def _():
                remote(
                    packed.at[slot],
                    out_ref.at[:, my_band],
                    out_send.at[slot],
                    out_recv.at[my_band],
                    core * slabs + slot,
                ).wait_send()

            return carry

        lax.fori_loop(0, slabs, drain, 0)


def per_device(bands, potential, table, kweight, lowest, cut, upper, fermi):
    n = lax.axis_size("grid")
    members_k = lax.axis_size("kpt")
    planes = bands.shape[3]
    parts = jnp.asarray(np.stack(third_parts()))
    pieces = 2 * planes
    flat = pieces * CHUNKS

    raw = bands[0].transpose(0, 2, 1, 3).reshape(pieces, BANDS, CHUNKS, LANES)
    raw = with_layout_constraint(raw, Layout((0, 2, 1, 3)))
    raw = raw.transpose(0, 2, 1, 3).reshape(flat, BANDS, 1, LANES)

    vmem, smem = pltpu.VMEM, pltpu.SMEM
    anywhere = pl.BlockSpec(memory_space=pl.ANY)
    hbm = pl.BlockSpec(memory_space=pltpu.HBM)
    scalar = pl.BlockSpec(memory_space=smem)
    slabs = n // 2
    workers = 2 * BANDS
    total_planes = slabs * planes
    dma = pltpu.SemaphoreType.DMA
    f32 = jnp.float32
    out, energy, total = pl.pallas_call(
        functools.partial(kernel, n, members_k, planes),
        name="cheb",
        out_shape=(
            jax.ShapeDtypeStruct((flat, BANDS, 1, LANES), f32),
            jax.ShapeDtypeStruct((1, BANDS), f32),
            jax.ShapeDtypeStruct((1, 1), f32),
        ),
        in_specs=[anywhere] * 6 + [hbm] * 3,
        out_specs=(hbm, scalar, scalar),
        scratch_shapes=[
            smem((1, 3), jnp.int32),
            smem((1,), f32),
            smem((1,), f32),
            smem((1,), f32),
            smem((1,), f32),
            smem((1,), f32),
            vmem((BANDS, flat, 1, LANES), f32),
            vmem((planes, SIDE * SIDE), f32),
            vmem((3, LANES, LANES), f32),
            vmem((total_planes + 2 * planes, ROWS, LANES), f32),
            vmem((total_planes + 2 * planes, ROWS, LANES), f32),
            vmem((total_planes + 2 * planes, ROWS, LANES), f32),
            vmem((2 * LANES, 2 * LANES), jnp.bfloat16),
            vmem((total_planes, SIDE, LANES), f32),
            vmem((slabs, flat, 1, LANES), f32),
            vmem((slabs, planes, SIDE * SIDE), f32),
            vmem((2, planes, SIDE, LANES), f32),
            vmem((2 * planes, SIDE, LANES), f32),
            vmem((slabs, flat, 1, LANES), f32),
            vmem((workers, 1, LANES), f32),
            vmem((members_k, 1, LANES), f32),
            dma((10,)),
            dma((BANDS,)),
            dma((slabs,)),
            dma((BANDS,)),
            dma((slabs,)),
            dma((2,)),
            dma((2, 2)),
            dma((slabs,)),
            dma((BANDS,)),
            dma((n,)),
            dma((workers,)),
            dma((members_k,)),
            dma((members_k,)),
        ],
        compiler_params=pltpu.CompilerParams(
            collective_id=0, has_side_effects=True, vmem_limit_bytes=48 * 1024 * 1024
        ),
    )(table, kweight, lowest, cut, upper, fermi, raw, potential, parts)
    filtered = out.reshape(pieces, CHUNKS, BANDS, LANES).transpose(0, 2, 1, 3)
    filtered = filtered.reshape(2, planes, BANDS, SIDE * SIDE).transpose(0, 2, 1, 3)[None]
    return filtered, energy, total[0]


def solution(mesh):
    in_specs = (
        P("kpt", None, None, "grid", None),
        P("grid", None),
        P("kpt", None),
        P("kpt"),
        P("kpt"),
        P("kpt"),
        P("kpt"),
        P(),
    )
    out_specs = (P("kpt", None, None, "grid", None), P("kpt", None), P())
    return jax.shard_map(
        per_device, mesh=mesh, in_specs=in_specs, out_specs=out_specs, check_vma=False
    )
```

```python
import functools

import jax
import jax.numpy as jnp
import numpy as np
from jax import lax
from jax.experimental import pallas as pl
from jax.experimental.layout import Layout, with_layout_constraint
from jax.experimental.pallas import tpu as pltpu
from jax.sharding import PartitionSpec as P

SIDE = 48
DEGREE = 6
PHASE_DIVISOR = 8
REACH = 6
LANES = 128
USED = 2 * SIDE
PAD = 8
ROWS = SIDE + 2 * PAD
TILES = SIDE // 8
CHUNKS = SIDE * SIDE // LANES
PER_TILE = CHUNKS // TILES
BANDS = 2

coefficients = (
    -5369.0 / 1800.0,
    12.0 / 7.0,
    -15.0 / 56.0,
    10.0 / 189.0,
    -1.0 / 112.0,
    2.0 / 1925.0,
    -1.0 / 16632.0,
)
smearing = 0.5
MESH = pl.DeviceIdType.MESH


def kernel(
    n,
    members_k,
    planes,
    table_ref,
    kweight_hbm,
    lowest_hbm,
    cut_hbm,
    upper_hbm,
    fermi_hbm,
    bands_hbm,
    pot_hbm,
    out_ref,
    energy_ref,
    total_ref,
    kweight_ref,
    lowest_ref,
    cut_ref,
    upper_ref,
    fermi_ref,
    own,
    own_pot,
    field_0,
    field_1,
    field_2,
    mat_ref,
    mixed,
    potential,
    stage,
    stage_pot,
    turned,
    partial,
    rolled,
    packed,
    part,
    part_k,
    load_sem,
    send,
    recv,
    send_pot,
    recv_pot,
    pass_sem,
    halo_send,
    halo_recv,
    out_send,
    out_recv,
    send_red,
    recv_red,
    send_k,
    recv_k,
):
    fields = (field_0, field_1, field_2)
    chips = n // 2
    slabs = n // 2
    total_planes = slabs * planes
    stride = chips // BANDS
    workers = 2 * BANDS

    def worker(b, half):
        return 2 * stride * b + half

    me = lax.axis_index("grid")
    kpt = lax.axis_index("kpt")
    core = lax.rem(me, 2)
    partner = me + 1 - 2 * core
    is_worker = lax.rem(lax.div(me, 2), stride) == 0
    my_band = lax.div(lax.div(me, 2), stride)
    my_place = 2 * my_band + core
    my_half = lax.div(me, slabs)
    my_slot = lax.rem(me, slabs)

    loads = [
        pltpu.make_async_copy(src, dst, load_sem.at[i])
        for i, (src, dst) in enumerate(
            (
                (kweight_hbm, kweight_ref),
                (lowest_hbm, lowest_ref),
                (cut_hbm, cut_ref),
                (upper_hbm, upper_ref),
                (fermi_hbm, fermi_ref),
                (pot_hbm, own_pot),
                (bands_hbm.at[:, 0], own.at[0]),
                (bands_hbm.at[:, 1], own.at[1]),
            )
        )
    ]
    for load in loads[::-1]:
        load.start()

    barrier = pltpu.get_barrier_semaphore()

    def greet(target_k, target):
        pl.semaphore_signal(barrier, inc=1, device_id=(target_k, target), device_id_type=MESH)

    for d in range(1, members_k):
        greet(lax.rem(kpt + d, members_k), me)

    @pl.when(is_worker)
    def _():
        for d in range(1, n):
            greet(kpt, lax.rem(me + d, n))

    @pl.when(jnp.logical_not(is_worker))
    def _():
        for w in range(workers):
            greet(kpt, worker(w // 2, w % 2))

    for load in loads[5:]:
        load.wait()
    pl.semaphore_wait(
        barrier, jnp.where(is_worker, n - 1 + members_k - 1, workers + members_k - 1)
    )

    def remote(src, dst, ssem, rsem, target):
        return pltpu.make_async_remote_copy(
            src_ref=src,
            dst_ref=dst,
            send_sem=ssem,
            recv_sem=rsem,
            device_id=(kpt, target),
            device_id_type=MESH,
        )

    def deliver(i):
        b = 1 - my_half if i == 0 else my_half
        target = worker(b, my_half)
        wave = remote(own.at[b], stage.at[my_slot], send.at[i], recv.at[my_slot], target)
        pot = remote(own_pot, stage_pot.at[my_slot], send_pot.at[i], recv_pot.at[my_slot], target)
        return wave, pot, target

    gives_pot = lax.rem(my_slot, members_k) == kpt
    for i in range(BANDS):
        wave, pot, target = deliver(i)

        @pl.when((target != me) & gives_pot)
        def _():
            pot.start()

    for i in range(BANDS):
        wave, pot, target = deliver(i)

        @pl.when(target != me)
        def _():
            wave.start()

    def pass_pot(slot, d):
        return pltpu.make_async_remote_copy(
            src_ref=stage_pot.at[slot],
            dst_ref=stage_pot.at[slot],
            send_sem=pass_sem.at[slot, d],
            recv_sem=recv_pot.at[slot],
            device_id=(lax.rem(kpt + d, members_k), me),
            device_id_type=MESH,
        )

    def land_pot(slot):
        here = stage_pot.at[slot]
        remote(here, here, send_pot.at[0], recv_pot.at[slot], partner).wait_recv()

    lane = lax.broadcasted_iota(jnp.int32, (8, LANES), 1)
    row = lax.broadcasted_iota(jnp.int32, (8, LANES), 0)
    first = lane < SIDE
    used = lane < USED
    zero = jnp.zeros((8, LANES), jnp.float32)

    def turn(v, cosine, sine):
        other = jnp.where(first, pltpu.roll(v, LANES - SIDE, 1), pltpu.roll(v, SIDE, 1))
        signed = jnp.where(used, jnp.where(first, -sine, sine), 0.0)
        return cosine * v + signed * other

    def spread(scalar):
        return jnp.full((8, LANES), scalar)

    for load in loads[:5]:
        load.wait()

    low_end, cut_end, high_end = (spread(r[0]) for r in (lowest_ref, cut_ref, upper_ref))
    half_width = (high_end - cut_end) / 2.0
    centre = (high_end + cut_end) / 2.0

    @pl.when(is_worker)
    def _():
        def phase(d):
            numerator = spread(table_ref[0, d])
            cosine, sine = jnp.ones((8, LANES), jnp.float32), zero
            for i in range(1, PHASE_DIVISOR):
                here = numerator == i
                angle = 2.0 * np.pi * i / PHASE_DIVISOR
                cosine = jnp.where(here, float(np.cos(angle)), cosine)
                sine = jnp.where(here, float(np.sin(angle)), sine)
            return cosine, sine

        cos_x, sin_x = phase(0)
        cos_y, sin_y = phase(1)
        cos_z, sin_z = phase(2)
        at_low = spread(core) == 0
        side_turn = (
            (jnp.where(at_low, cos_x, 1.0), jnp.where(at_low, sin_x, 0.0)),
            (jnp.where(at_low, 1.0, cos_x), jnp.where(at_low, 0.0, -sin_x)),
        )
        first_sigma = half_width / (low_end - centre)
        sigma = first_sigma
        final_scale = first_sigma
        for degree in range(1, DEGREE):
            sigma = 1.0 / (2.0 / first_sigma - sigma)
            final_scale = final_scale * sigma
        scale = 2.0 / half_width
        weights = [scale * (-0.5 * c) for c in coefficients]

        for r in range(LANES // 8):
            target = row + 8 * r
            target_z = jnp.where(target < SIDE, target, target - SIDE)
            source_z = jnp.where(first, lane, lane - SIDE)
            gap = target_z - source_z
            apart = jnp.abs(gap)
            near, wrap = zero, zero
            for j in range(1, REACH + 1):
                near = jnp.where(apart == j, weights[j], near)
                wrap = jnp.where(apart == SIDE - j, weights[j], wrap)
            across_sign = jnp.where((gap < 0) == (target < SIDE), sin_z, -sin_z)
            same = (target < SIDE) == first
            entry = jnp.where(same, near + cos_z * wrap, across_sign * wrap)
            entry = jnp.where(used & (target < USED), entry, 0.0)
            mixed[pl.ds(8 * r, 8), :] = entry
        for r in range(LANES // 16):
            rows = pl.ds(16 * r, 16)
            entry = mixed[rows, :]
            high = entry.astype(jnp.bfloat16)
            rest = (entry - high.astype(jnp.float32)).astype(jnp.bfloat16)
            lower = pl.ds(LANES + 16 * r, 16)
            mat_ref[rows, pl.ds(0, LANES)] = high
            mat_ref[rows, pl.ds(LANES, LANES)] = rest
            mat_ref[lower, pl.ds(0, LANES)] = high
            mat_ref[lower, pl.ds(LANES, LANES)] = jnp.zeros_like(high)

        def clear(p, carry):
            for t in range(TILES):
                field_2[planes + p, pl.ds(PAD + 8 * t, 8), :] = zero
            return carry

        lax.fori_loop(0, total_planes, clear, 0)

        def put(f, plane, t, v):
            f[plane, pl.ds(PAD + 8 * t, 8), :] = v
            if t == 0:
                f[plane, pl.ds(PAD + SIDE, 8), :] = turn(v, cos_y, sin_y)
            if t == TILES - 1:
                f[plane, pl.ds(0, 8), :] = turn(v, cos_y, -sin_y)

        def ordering(part_index):
            begin = SIDE * lax.rem(5 * row + part_index, 8)
            which = lax.shift_right_logical(begin + ((lane - begin) & (LANES - 1)), 7)
            return which, lax.rem(5 * row + 3 * part_index, 8)

        orders = [ordering(i) for i in range(2)]

        def lay(load, part_index):
            which, back = orders[part_index]
            ahead = [jnp.broadcast_to(load(i), (8, LANES)) for i in range(PER_TILE)]
            v = jnp.where(which == 0, ahead[0], jnp.where(which == 1, ahead[1], ahead[2]))
            v = pltpu.roll(v, 0, 1, stride=16, stride_axis=0)
            return jnp.take_along_axis(v, back, axis=0)

        flat = stage.reshape(slabs, 2 * planes * CHUNKS, LANES)

        def unpack(slot):
            for p in range(planes):
                for t in range(TILES):
                    def rows_of(part_index):
                        base = (part_index * planes + p) * CHUNKS + PER_TILE * t
                        return lay(
                            lambda i: flat[slot, pl.ds(base + i, 1), :], part_index
                        )

                    v = jnp.where(first, rows_of(0), jnp.where(used, rows_of(1), 0.0))
                    put(field_0, planes + slot * planes + p, t, v)

        def unpack_pot(slot):
            for p in range(planes):
                for t in range(TILES):
                    v = lay(
                        lambda i: stage_pot[
                            slot, pl.ds(p, 1), pl.ds((PER_TILE * t + i) * LANES, LANES)
                        ],
                        0,
                    )
                    v = (v - 1.5 * coefficients[0] - centre) * scale
                    v = jnp.where(first, v, jnp.where(used, pltpu.roll(v, SIDE, 1), 0.0))
                    potential[slot * planes + p, pl.ds(8 * t, 8), :] = v

        def take(i, carry):
            slot = jnp.where(my_band == 0, jnp.where(core == 0, i, slabs - 1 - i), jnp.where(core == 0, slabs - 1 - i, i))

            @pl.when(half_base + slot != me)
            def _():
                remote(stage.at[slot], stage.at[slot], send.at[0], recv.at[slot], partner).wait_recv()

            unpack(slot)
            return carry

        half_base = core * slabs

        @pl.when(my_half == core)
        def _():
            own_flat = own.reshape(BANDS, 2 * planes * CHUNKS, LANES)
            for r in range(2 * planes * CHUNKS // 8):
                flat[my_slot, pl.ds(8 * r, 8), :] = own_flat[my_band, pl.ds(8 * r, 8), :]

            @pl.when(gives_pot)
            def _():
                for c in range(CHUNKS):
                    part_of = pl.ds(c * LANES, LANES)
                    stage_pot[my_slot, :, part_of] = own_pot[:, part_of]

        def spread_pot(slot, carry):
            @pl.when(lax.rem(slot, members_k) == kpt)
            def _():
                @pl.when(half_base + slot != me)
                def _():
                    land_pot(slot)

                for d in range(1, members_k):
                    pass_pot(slot, d).start()

            return carry

        lax.fori_loop(0, slabs, spread_pot, 0)
        lax.fori_loop(0, slabs, take, 0)

        body = pl.ds(PAD, SIDE)

        def halo(f, side, parity):
            there = total_planes + planes if side == 0 else 0
            return remote(
                turned.at[side],
                f.at[pl.ds(there, planes), body, :],
                halo_send.at[side],
                halo_recv.at[1 - side, parity],
                partner,
            )

        def hold(side, p, t, v):
            turned[side, p, pl.ds(8 * t, 8), :] = turn(v, *side_turn[side])

        for side in range(2):
            base = planes if side == 0 else total_planes

            for p in range(planes):
                for t in range(TILES):
                    hold(side, p, t, field_0[base + p, pl.ds(PAD + 8 * t, 8), :])
            halo(field_0, side, 0).start()

        def take_pot(i, carry):
            slot = lax.rem(kpt + i, slabs)

            @pl.when(lax.rem(slot, members_k) != kpt)
            def _():
                land_pot(slot)

            unpack_pot(slot)
            return carry

        lax.fori_loop(0, slabs, take_pot, 0)

        def third_of(f, spans):
            rows = jnp.concatenate(
                [f[planes + q, body, :] for start in spans for q in qs(start)], axis=0
            )
            high = rows.astype(jnp.bfloat16)
            rest = (rows - high.astype(jnp.float32)).astype(jnp.bfloat16)
            both = jnp.concatenate([high, rest], axis=1)
            third = jnp.dot(both, mat_ref[...], preferred_element_type=jnp.float32)
            return third[:, :LANES] + third[:, LANES:]

        def qs(start):
            return [start + p for p in range(planes)]

        def apply(f, spans, sides):
            third = third_of(f, spans)
            for i, start in enumerate(spans):
                side = sides[i]
                for t in range(TILES):
                    tile = pl.ds(PAD + 8 * t, 8)
                    low = planes if side == 0 else 0
                    high = 2 * planes if side == 1 else 3 * planes
                    window = [
                        f[start + q, tile, :] if low <= q < high else None
                        for q in range(3 * planes)
                    ]
                    for p in range(planes):
                        value = window[planes + p]
                        at = (i * planes + p) * SIDE + 8 * t
                        total = third[at : at + 8, :]
                        total = total + value * potential[start + p, pl.ds(8 * t, 8), :]
                        for j in range(1, REACH + 1):
                            above = f[planes + start + p, pl.ds(PAD + 8 * t + j, 8), :]
                            below = f[planes + start + p, pl.ds(PAD + 8 * t - j, 8), :]
                            around = above + below
                            for q in (planes + p + j, planes + p - j):
                                if window[q] is not None:
                                    around = around + window[q]
                            total = total + weights[j] * around
                        yield i, p, start + p, t, tile, value, total

        def finish(f, start, side):
            for t in range(TILES):
                tile = pl.ds(PAD + 8 * t, 8)
                there = total_planes + planes if side == 1 else 0
                window = [f[there + q, tile, :] for q in range(planes)]
                for p in range(planes):
                    total = partial[side * planes + p, pl.ds(8 * t, 8), :]
                    for j in range(1, REACH + 1):
                        q = p + j - planes if side == 1 else planes + p - j
                        if 0 <= q < planes:
                            total = total + weights[j] * window[q]
                    yield p, start + p, t, tile, total

        outer = (0, total_planes - planes)

        def begin(f):
            for i, p, _, t, _, _, total in apply(f, outer, (0, 1)):
                partial[i * planes + p, pl.ds(8 * t, 8), :] = total

        def await_halos(f, parity):
            for side in range(2):
                halo(f, side, parity).wait_send()
            for side in range(2):
                there = total_planes + planes if side == 1 else 0
                landed = f.at[pl.ds(there, planes), body, :]
                remote(
                    landed, landed, halo_send.at[side], halo_recv.at[side, parity], partner
                ).wait_recv()

        def step(m, c):
            now, then, before = (fields[(c + i) % 3] for i in range(3))
            gain = jnp.where(m == 1, 0.5, 1.0)

            def settle(plane, t, tile, total):
                following = gain * total - before[planes + plane, tile, :]
                put(then, planes + plane, t, following)
                return following

            begin(now)

            def inner(k, carry):
                start = planes + 2 * planes * k
                spans = (start, start + planes)
                for _, _, plane, t, tile, _, total in apply(now, spans, (None, None)):
                    settle(plane, t, tile, total)
                return carry

            lax.fori_loop(0, slabs // 2 - 1, inner, 0)
            parity = lax.rem(m - 1, 2)
            await_halos(now, parity)
            for side in range(2):
                for p, plane, t, tile, total in finish(now, outer[side], side):
                    hold(side, p, t, settle(plane, t, tile, total))
                halo(then, side, 1 - parity).start()

        def three(r, carry):
            for c in range(3):
                step(3 * r + c + 1, c)
            return carry

        lax.fori_loop(0, DEGREE // 3, three, 0)
        final = field_0

        flat_packed = packed.reshape(slabs, 2 * planes * CHUNKS, LANES)
        gather_rows = [lax.rem(3 * row + i, 8) for i in range(2)]
        lane6 = lax.broadcasted_iota(jnp.int32, (TILES, LANES), 1)

        def give(slot):
            return remote(
                packed.at[slot],
                out_ref.at[:, my_band],
                out_send.at[slot],
                out_recv.at[my_band],
                core * slabs + slot,
            )

        def give_here(slot):
            return pltpu.make_async_copy(
                packed.at[slot], out_ref.at[:, my_band], out_recv.at[my_band]
            )

        def pack(i, carry):
            slot = jnp.where(core == 0, i, slabs - 1 - i)

            for p in range(planes):
                plane = planes + slot * planes + p
                for part_index in range(2):
                    lot = 2 * p + part_index
                    for t in range(TILES):
                        v = final[plane, pl.ds(PAD + 8 * t, 8), :] * final_scale
                        v = jnp.take_along_axis(v, gather_rows[part_index], axis=0)
                        v = pltpu.roll(v, 0, 1, stride=16, stride_axis=0)
                        rolled[lot, pl.ds(8 * t, 8), :] = v
            for p in range(planes):
                for part_index in range(2):
                    lot = 2 * p + part_index
                    picks = [
                        rolled[lot, pl.ds((3 * i + 5 * part_index) % 8, TILES, stride=8), :]
                        for i in range(8)
                    ]

                    def choose(*ends):
                        start = ends[0]
                        v = picks[start + len(ends) - 1]
                        for i in range(len(ends) - 2, -1, -1):
                            v = jnp.where(lane6 < ends[i + 1], picks[start + i], v)
                        return v

                    rows = (choose(0, 48, 96), choose(2, 16, 64, 112), choose(5, 32, 80))
                    base = (part_index * planes + p) * CHUNKS
                    for j in range(PER_TILE):
                        flat_packed[slot, pl.ds(base + j, TILES, stride=PER_TILE), :] = rows[j]

            @pl.when(core * slabs + slot != me)
            def _():
                give(slot).start()

            @pl.when(core * slabs + slot == me)
            def _():
                give_here(slot).start()

            return carry

        lax.fori_loop(0, slabs, pack, 0)

        begin(final)

        def gather_up(sums, t, value, total):
            tops, bottoms = sums
            tops[t % 2] = tops[t % 2] + value * total
            bottoms[t % 2] = bottoms[t % 2] + value * value

        def inner_sums(k, carry):
            sums = list(carry[0]), list(carry[1])
            start = planes + 2 * planes * k
            for _, _, _, t, _, value, total in apply(
                final, (start, start + planes), (None, None)
            ):
                gather_up(sums, t, value, total)
            return tuple(sums[0]), tuple(sums[1])

        carry = ((zero, zero), (zero, zero))
        carry = lax.fori_loop(0, slabs // 2 - 1, inner_sums, carry)
        tops, bottoms = sums = list(carry[0]), list(carry[1])
        await_halos(final, DEGREE % 2)
        for side in range(2):
            for _, plane, t, tile, total in finish(final, outer[side], side):
                gather_up(sums, t, final[planes + plane, tile, :], total)
        top = jnp.sum(tops[0] + tops[1], keepdims=True)
        bottom = jnp.sum(bottoms[0] + bottoms[1], keepdims=True)
        left = lax.broadcasted_iota(jnp.int32, (1, LANES), 1) < LANES // 2
        part[my_place] = jnp.where(left, top, bottom)
        for d in range(1, n):
            remote(
                part.at[my_place],
                part.at[my_place],
                send_red.at[d],
                recv_red.at[my_place],
                lax.rem(me + d, n),
            ).start()

    for w in range(workers):

        @pl.when(me != worker(w // 2, w % 2))
        def _():
            remote(part.at[w], part.at[w], send_red.at[0], recv_red.at[w], partner).wait_recv()

    kweight, fermi = kweight_ref[0], fermi_ref[0]
    e_half, c_half = half_width[0:1, :], centre[0:1, :]
    term = jnp.zeros((1, LANES), jnp.float32)
    for b in range(BANDS):
        both = part[2 * b] + part[2 * b + 1]
        energy = (0.5 * e_half) * (both / pltpu.roll(both, LANES // 2, 1)) + c_half
        energy_ref[0, b] = energy[0, 0]
        term = term + energy / (1.0 + jnp.exp((energy - fermi) / smearing))
    part_k[kpt] = kweight * term

    def across(d, source, target):
        return pltpu.make_async_remote_copy(
            src_ref=part_k.at[source],
            dst_ref=part_k.at[source],
            send_sem=send_k.at[d],
            recv_sem=recv_k.at[source],
            device_id=(target, me),
            device_id_type=MESH,
        )

    for d in range(1, members_k):
        across(d, kpt, lax.rem(kpt + d, members_k)).start()
    for d in range(1, members_k):
        source = lax.rem(kpt + d, members_k)
        across(d, source, source).wait_recv()
    grand = jnp.zeros((1, LANES), jnp.float32)
    for k in range(members_k):
        grand = grand + part_k[k]
    total_ref[0, 0] = grand[0, 0]

    for b in range(BANDS):
        landing = out_ref.at[:, b]
        remote(landing, landing, out_send.at[0], out_recv.at[b], partner).wait_recv()

    for i in range(BANDS):
        wave, pot, target = deliver(i)

        @pl.when(target != me)
        def _():
            wave.wait_send()

        @pl.when((target != me) & gives_pot)
        def _():
            pot.wait_send()

    for d in range(1, members_k):
        across(d, kpt, lax.rem(kpt + d, members_k)).wait_send()

    @pl.when(is_worker)
    def _():
        for d in range(1, n):
            remote(
                part.at[my_place],
                part.at[my_place],
                send_red.at[d],
                recv_red.at[my_place],
                lax.rem(me + d, n),
            ).wait_send()

        def drain(slot, carry):
            @pl.when(core * slabs + slot != me)
            def _():
                remote(
                    packed.at[slot],
                    out_ref.at[:, my_band],
                    out_send.at[slot],
                    out_recv.at[my_band],
                    core * slabs + slot,
                ).wait_send()

            return carry

        lax.fori_loop(0, slabs, drain, 0)

        def drain_pot(slot, carry):
            @pl.when(lax.rem(slot, members_k) == kpt)
            def _():
                for d in range(1, members_k):
                    pass_pot(slot, d).wait_send()

            return carry

        lax.fori_loop(0, slabs, drain_pot, 0)


def per_device(bands, potential, table, kweight, lowest, cut, upper, fermi):
    n = lax.axis_size("grid")
    members_k = lax.axis_size("kpt")
    planes = bands.shape[3]
    pieces = 2 * planes
    flat = pieces * CHUNKS

    raw = bands[0].transpose(0, 2, 1, 3).reshape(pieces, BANDS, CHUNKS, LANES)
    raw = with_layout_constraint(raw, Layout((0, 2, 1, 3)))
    raw = raw.transpose(0, 2, 1, 3).reshape(flat, BANDS, 1, LANES)

    vmem, smem = pltpu.VMEM, pltpu.SMEM
    anywhere = pl.BlockSpec(memory_space=pl.ANY)
    hbm = pl.BlockSpec(memory_space=pltpu.HBM)
    scalar = pl.BlockSpec(memory_space=smem)
    slabs = n // 2
    workers = 2 * BANDS
    total_planes = slabs * planes
    dma = pltpu.SemaphoreType.DMA
    f32 = jnp.float32
    out, energy, total = pl.pallas_call(
        functools.partial(kernel, n, members_k, planes),
        name="cheb",
        out_shape=(
            jax.ShapeDtypeStruct((flat, BANDS, 1, LANES), f32),
            jax.ShapeDtypeStruct((1, BANDS), f32),
            jax.ShapeDtypeStruct((1, 1), f32),
        ),
        in_specs=[scalar] + [hbm] * 7,
        out_specs=(hbm, scalar, scalar),
        scratch_shapes=[
            smem((1,), f32),
            smem((1,), f32),
            smem((1,), f32),
            smem((1,), f32),
            smem((1,), f32),
            vmem((BANDS, flat, 1, LANES), f32),
            vmem((planes, SIDE * SIDE), f32),
            vmem((total_planes + 2 * planes, ROWS, LANES), f32),
            vmem((total_planes + 2 * planes, ROWS, LANES), f32),
            vmem((total_planes + 2 * planes, ROWS, LANES), f32),
            vmem((2 * LANES, 2 * LANES), jnp.bfloat16),
            vmem((LANES, LANES), f32),
            vmem((total_planes, SIDE, LANES), f32),
            vmem((slabs, flat, 1, LANES), f32),
            vmem((slabs, planes, SIDE * SIDE), f32),
            vmem((2, planes, SIDE, LANES), f32),
            vmem((2 * planes, SIDE, LANES), f32),
            vmem((2 * planes, SIDE, LANES), f32),
            vmem((slabs, flat, 1, LANES), f32),
            vmem((workers, 1, LANES), f32),
            vmem((members_k, 1, LANES), f32),
            dma((8,)),
            dma((BANDS,)),
            dma((slabs,)),
            dma((BANDS,)),
            dma((slabs,)),
            dma((slabs, members_k)),
            dma((2,)),
            dma((2, 2)),
            dma((slabs,)),
            dma((BANDS,)),
            dma((n,)),
            dma((workers,)),
            dma((members_k,)),
            dma((members_k,)),
        ],
        compiler_params=pltpu.CompilerParams(
            collective_id=0, has_side_effects=True, vmem_limit_bytes=62 * 1024 * 1024
        ),
    )(table, kweight, lowest, cut, upper, fermi, raw, potential)
    filtered = out.reshape(pieces, CHUNKS, BANDS, LANES).transpose(0, 2, 1, 3)
    filtered = filtered.reshape(2, planes, BANDS, SIDE * SIDE).transpose(0, 2, 1, 3)[None]
    return filtered, energy, total[0]


def solution(mesh):
    in_specs = (
        P("kpt", None, None, "grid", None),
        P("grid", None),
        P("kpt", None),
        P("kpt"),
        P("kpt"),
        P("kpt"),
        P("kpt"),
        P(),
    )
    out_specs = (P("kpt", None, None, "grid", None), P("kpt", None), P())
    return jax.shard_map(
        per_device, mesh=mesh, in_specs=in_specs, out_specs=out_specs, check_vma=False
    )
```

```python
import functools

import jax
import jax.numpy as jnp
import numpy as np
from jax import lax
from jax.experimental import pallas as pl
from jax.experimental.layout import Layout, with_layout_constraint
from jax.experimental.pallas import tpu as pltpu
from jax.sharding import PartitionSpec as P

SIDE = 48
DEGREE = 6
PHASE_DIVISOR = 8
REACH = 6
LANES = 128
USED = 2 * SIDE
PAD = 8
ROWS = SIDE + 2 * PAD
TILES = SIDE // 8
CHUNKS = SIDE * SIDE // LANES
PER_TILE = CHUNKS // TILES
BANDS = 2

coefficients = (
    -5369.0 / 1800.0,
    12.0 / 7.0,
    -15.0 / 56.0,
    10.0 / 189.0,
    -1.0 / 112.0,
    2.0 / 1925.0,
    -1.0 / 16632.0,
)
smearing = 0.5
MESH = pl.DeviceIdType.MESH


def kernel(
    n,
    members_k,
    planes,
    table_ref,
    kweight_hbm,
    lowest_hbm,
    cut_hbm,
    upper_hbm,
    fermi_hbm,
    bands_hbm,
    pot_hbm,
    out_ref,
    energy_ref,
    total_ref,
    kweight_ref,
    lowest_ref,
    cut_ref,
    upper_ref,
    fermi_ref,
    own,
    own_pot,
    field_0,
    field_1,
    field_2,
    mat_ref,
    mixed,
    potential,
    stage,
    stage_pot,
    turned,
    partial,
    rolled,
    packed,
    part,
    part_k,
    relay_in,
    relay_out,
    load_sem,
    send,
    recv,
    send_pot,
    recv_pot,
    pass_sem,
    halo_send,
    halo_recv,
    out_send,
    out_recv,
    send_red,
    recv_red,
    send_k,
    recv_k,
    relay_send,
    relay_recv,
):
    fields = (field_0, field_1, field_2)
    chips = n // 2
    slabs = n // 2
    total_planes = slabs * planes
    stride = chips // BANDS
    workers = 2 * BANDS

    def worker(b, half):
        return 2 * stride * b + half

    me = lax.axis_index("grid")
    kpt = lax.axis_index("kpt")
    core = lax.rem(me, 2)
    partner = me + 1 - 2 * core
    is_worker = lax.rem(lax.div(me, 2), stride) == 0
    my_band = lax.div(lax.div(me, 2), stride)
    my_place = 2 * my_band + core
    relay_on = chips == 2 * BANDS
    relayed = is_worker & (core == 1) if relay_on else jnp.bool_(False)
    my_half = lax.div(me, slabs)
    my_slot = lax.rem(me, slabs)

    loads = [
        pltpu.make_async_copy(src, dst, load_sem.at[i])
        for i, (src, dst) in enumerate(
            (
                (kweight_hbm, kweight_ref),
                (lowest_hbm, lowest_ref),
                (cut_hbm, cut_ref),
                (upper_hbm, upper_ref),
                (fermi_hbm, fermi_ref),
                (pot_hbm, own_pot),
                (bands_hbm.at[:, 0], own.at[0]),
                (bands_hbm.at[:, 1], own.at[1]),
            )
        )
    ]
    for load in loads[::-1]:
        load.start()

    barrier = pltpu.get_barrier_semaphore()

    def greet(target_k, target):
        pl.semaphore_signal(barrier, inc=1, device_id=(target_k, target), device_id_type=MESH)

    for d in range(1, members_k):
        greet(lax.rem(kpt + d, members_k), me)

    @pl.when(is_worker)
    def _():
        for d in range(1, n):
            greet(kpt, lax.rem(me + d, n))

    @pl.when(jnp.logical_not(is_worker))
    def _():
        for w in range(workers):
            greet(kpt, worker(w // 2, w % 2))

    for load in loads[5:]:
        load.wait()
    pl.semaphore_wait(
        barrier, jnp.where(is_worker, n - 1 + members_k - 1, workers + members_k - 1)
    )

    def remote(src, dst, ssem, rsem, target):
        return pltpu.make_async_remote_copy(
            src_ref=src,
            dst_ref=dst,
            send_sem=ssem,
            recv_sem=rsem,
            device_id=(kpt, target),
            device_id_type=MESH,
        )

    def deliver(i):
        b = 1 - my_half if i == 0 else my_half
        target = worker(b, my_half)
        wave = remote(own.at[b], stage.at[my_slot], send.at[i], recv.at[my_slot], target)
        pot = remote(own_pot, stage_pot.at[my_slot], send_pot.at[i], recv_pot.at[my_slot], target)
        return wave, pot, target

    gives_pot = lax.rem(my_slot, members_k) == kpt
    for i in range(BANDS):
        wave, pot, target = deliver(i)

        @pl.when((target != me) & gives_pot)
        def _():
            pot.start()

    for i in range(BANDS):
        wave, pot, target = deliver(i)
        around = relayed if i == 0 else False

        @pl.when((target != me) & jnp.logical_not(around))
        def _():
            wave.start()

        if relay_on and i == 0:

            @pl.when(relayed)
            def _():
                remote(
                    own.at[1 - my_half], relay_in, send.at[0], relay_recv.at[0], lax.rem(me + n - 2, n)
                ).start()

    def pass_pot(slot, d):
        return pltpu.make_async_remote_copy(
            src_ref=stage_pot.at[slot],
            dst_ref=stage_pot.at[slot],
            send_sem=pass_sem.at[slot, d],
            recv_sem=recv_pot.at[slot],
            device_id=(lax.rem(kpt + d, members_k), me),
            device_id_type=MESH,
        )

    def land_pot(slot):
        here = stage_pot.at[slot]
        remote(here, here, send_pot.at[0], recv_pot.at[slot], partner).wait_recv()

    if relay_on:

        @pl.when(jnp.logical_not(is_worker) & (core == 1))
        def _():
            source, sink = lax.rem(me + 2, n), lax.rem(me + n - 2, n)
            half, slot = lax.div(source, slabs), lax.rem(source, slabs)
            band = lax.div(lax.div(source, 2), stride)
            remote(relay_in, relay_in, relay_send.at[0], relay_recv.at[0], partner).wait_recv()
            onward = remote(
                relay_in, stage.at[slot], relay_send.at[0], recv.at[slot], worker(1 - half, half)
            )
            onward.start()
            remote(relay_out, relay_out, relay_send.at[1], relay_recv.at[1], partner).wait_recv()
            homeward = remote(
                relay_out, out_ref.at[:, band], relay_send.at[1], out_recv.at[band], sink
            )
            homeward.start()
            onward.wait_send()
            homeward.wait_send()

    lane = lax.broadcasted_iota(jnp.int32, (8, LANES), 1)
    row = lax.broadcasted_iota(jnp.int32, (8, LANES), 0)
    first = lane < SIDE
    used = lane < USED
    zero = jnp.zeros((8, LANES), jnp.float32)

    def turn(v, cosine, sine):
        other = jnp.where(first, pltpu.roll(v, LANES - SIDE, 1), pltpu.roll(v, SIDE, 1))
        signed = jnp.where(used, jnp.where(first, -sine, sine), 0.0)
        return cosine * v + signed * other

    def spread(scalar):
        return jnp.full((8, LANES), scalar)

    for load in loads[:5]:
        load.wait()

    low_end, cut_end, high_end = (spread(r[0]) for r in (lowest_ref, cut_ref, upper_ref))
    half_width = (high_end - cut_end) / 2.0
    centre = (high_end + cut_end) / 2.0

    @pl.when(is_worker)
    def _():
        def phase(d):
            numerator = spread(table_ref[0, d])
            cosine, sine = jnp.ones((8, LANES), jnp.float32), zero
            for i in range(1, PHASE_DIVISOR):
                here = numerator == i
                angle = 2.0 * np.pi * i / PHASE_DIVISOR
                cosine = jnp.where(here, float(np.cos(angle)), cosine)
                sine = jnp.where(here, float(np.sin(angle)), sine)
            return cosine, sine

        cos_x, sin_x = phase(0)
        cos_y, sin_y = phase(1)
        cos_z, sin_z = phase(2)
        at_low = spread(core) == 0
        side_turn = (
            (jnp.where(at_low, cos_x, 1.0), jnp.where(at_low, sin_x, 0.0)),
            (jnp.where(at_low, 1.0, cos_x), jnp.where(at_low, 0.0, -sin_x)),
        )
        first_sigma = half_width / (low_end - centre)
        sigma = first_sigma
        final_scale = first_sigma
        for degree in range(1, DEGREE):
            sigma = 1.0 / (2.0 / first_sigma - sigma)
            final_scale = final_scale * sigma
        scale = 2.0 / half_width
        weights = [scale * (-0.5 * c) for c in coefficients]

        for r in range(LANES // 8):
            target = row + 8 * r
            target_z = jnp.where(target < SIDE, target, target - SIDE)
            source_z = jnp.where(first, lane, lane - SIDE)
            gap = target_z - source_z
            apart = jnp.abs(gap)
            near, wrap = zero, zero
            for j in range(1, REACH + 1):
                near = jnp.where(apart == j, weights[j], near)
                wrap = jnp.where(apart == SIDE - j, weights[j], wrap)
            across_sign = jnp.where((gap < 0) == (target < SIDE), sin_z, -sin_z)
            same = (target < SIDE) == first
            entry = jnp.where(same, near + cos_z * wrap, across_sign * wrap)
            entry = jnp.where(used & (target < USED), entry, 0.0)
            mixed[pl.ds(8 * r, 8), :] = entry
        for r in range(LANES // 16):
            rows = pl.ds(16 * r, 16)
            entry = mixed[rows, :]
            high = entry.astype(jnp.bfloat16)
            rest = (entry - high.astype(jnp.float32)).astype(jnp.bfloat16)
            lower = pl.ds(LANES + 16 * r, 16)
            mat_ref[rows, pl.ds(0, LANES)] = high
            mat_ref[rows, pl.ds(LANES, LANES)] = rest
            mat_ref[lower, pl.ds(0, LANES)] = high
            mat_ref[lower, pl.ds(LANES, LANES)] = jnp.zeros_like(high)

        def clear(p, carry):
            for t in range(TILES):
                field_2[planes + p, pl.ds(PAD + 8 * t, 8), :] = zero
            return carry

        lax.fori_loop(0, total_planes, clear, 0)

        def put(f, plane, t, v):
            f[plane, pl.ds(PAD + 8 * t, 8), :] = v
            if t == 0:
                f[plane, pl.ds(PAD + SIDE, 8), :] = turn(v, cos_y, sin_y)
            if t == TILES - 1:
                f[plane, pl.ds(0, 8), :] = turn(v, cos_y, -sin_y)

        def ordering(part_index):
            begin = SIDE * lax.rem(5 * row + part_index, 8)
            which = lax.shift_right_logical(begin + ((lane - begin) & (LANES - 1)), 7)
            return which, lax.rem(5 * row + 3 * part_index, 8)

        orders = [ordering(i) for i in range(2)]

        def lay(load, part_index):
            which, back = orders[part_index]
            ahead = [jnp.broadcast_to(load(i), (8, LANES)) for i in range(PER_TILE)]
            v = jnp.where(which == 0, ahead[0], jnp.where(which == 1, ahead[1], ahead[2]))
            v = pltpu.roll(v, 0, 1, stride=16, stride_axis=0)
            return jnp.take_along_axis(v, back, axis=0)

        flat = stage.reshape(slabs, 2 * planes * CHUNKS, LANES)

        def unpack(slot):
            for p in range(planes):
                for t in range(TILES):
                    def rows_of(part_index):
                        base = (part_index * planes + p) * CHUNKS + PER_TILE * t
                        return lay(
                            lambda i: flat[slot, pl.ds(base + i, 1), :], part_index
                        )

                    v = jnp.where(first, rows_of(0), jnp.where(used, rows_of(1), 0.0))
                    put(field_0, planes + slot * planes + p, t, v)

        def unpack_pot(slot):
            for p in range(planes):
                for t in range(TILES):
                    v = lay(
                        lambda i: stage_pot[
                            slot, pl.ds(p, 1), pl.ds((PER_TILE * t + i) * LANES, LANES)
                        ],
                        0,
                    )
                    v = (v - 1.5 * coefficients[0] - centre) * scale
                    v = jnp.where(first, v, jnp.where(used, pltpu.roll(v, SIDE, 1), 0.0))
                    potential[slot * planes + p, pl.ds(8 * t, 8), :] = v

        def take(i, carry):
            slot = jnp.where(my_band == 0, jnp.where(core == 0, i, slabs - 1 - i), jnp.where(core == 0, slabs - 1 - i, i))

            @pl.when(half_base + slot != me)
            def _():
                remote(stage.at[slot], stage.at[slot], send.at[0], recv.at[slot], partner).wait_recv()

            unpack(slot)
            return carry

        half_base = core * slabs

        @pl.when(my_half == core)
        def _():
            own_flat = own.reshape(BANDS, 2 * planes * CHUNKS, LANES)
            for r in range(2 * planes * CHUNKS // 8):
                flat[my_slot, pl.ds(8 * r, 8), :] = own_flat[my_band, pl.ds(8 * r, 8), :]

            @pl.when(gives_pot)
            def _():
                for c in range(CHUNKS):
                    part_of = pl.ds(c * LANES, LANES)
                    stage_pot[my_slot, :, part_of] = own_pot[:, part_of]

        def spread_pot(slot, carry):
            @pl.when(lax.rem(slot, members_k) == kpt)
            def _():
                @pl.when(half_base + slot != me)
                def _():
                    land_pot(slot)

                for d in range(1, members_k):
                    pass_pot(slot, d).start()

            return carry

        lax.fori_loop(0, slabs, spread_pot, 0)
        lax.fori_loop(0, slabs, take, 0)

        body = pl.ds(PAD, SIDE)

        def halo(f, side, parity):
            there = total_planes + planes if side == 0 else 0
            return remote(
                turned.at[side],
                f.at[pl.ds(there, planes), body, :],
                halo_send.at[side],
                halo_recv.at[1 - side, parity],
                partner,
            )

        def hold(side, p, t, v):
            turned[side, p, pl.ds(8 * t, 8), :] = turn(v, *side_turn[side])

        for side in range(2):
            base = planes if side == 0 else total_planes

            for p in range(planes):
                for t in range(TILES):
                    hold(side, p, t, field_0[base + p, pl.ds(PAD + 8 * t, 8), :])
            halo(field_0, side, 0).start()

        def take_pot(i, carry):
            slot = lax.rem(kpt + i, slabs)

            @pl.when(lax.rem(slot, members_k) != kpt)
            def _():
                land_pot(slot)

            unpack_pot(slot)
            return carry

        lax.fori_loop(0, slabs, take_pot, 0)

        def third_of(f, spans):
            rows = jnp.concatenate(
                [f[planes + q, body, :] for start in spans for q in qs(start)], axis=0
            )
            high = rows.astype(jnp.bfloat16)
            rest = (rows - high.astype(jnp.float32)).astype(jnp.bfloat16)
            both = jnp.concatenate([high, rest], axis=1)
            third = jnp.dot(both, mat_ref[...], preferred_element_type=jnp.float32)
            return third[:, :LANES] + third[:, LANES:]

        def qs(start):
            return [start + p for p in range(planes)]

        def apply(f, spans, sides):
            third = third_of(f, spans)
            for i, start in enumerate(spans):
                side = sides[i]
                for t in range(TILES):
                    tile = pl.ds(PAD + 8 * t, 8)
                    low = planes if side == 0 else 0
                    high = 2 * planes if side == 1 else 3 * planes
                    window = [
                        f[start + q, tile, :] if low <= q < high else None
                        for q in range(3 * planes)
                    ]
                    for p in range(planes):
                        value = window[planes + p]
                        at = (i * planes + p) * SIDE + 8 * t
                        total = third[at : at + 8, :]
                        total = total + value * potential[start + p, pl.ds(8 * t, 8), :]
                        for j in range(1, REACH + 1):
                            above = f[planes + start + p, pl.ds(PAD + 8 * t + j, 8), :]
                            below = f[planes + start + p, pl.ds(PAD + 8 * t - j, 8), :]
                            around = above + below
                            for q in (planes + p + j, planes + p - j):
                                if window[q] is not None:
                                    around = around + window[q]
                            total = total + weights[j] * around
                        yield i, p, start + p, t, tile, value, total

        def finish(f, start, side):
            for t in range(TILES):
                tile = pl.ds(PAD + 8 * t, 8)
                there = total_planes + planes if side == 1 else 0
                window = [f[there + q, tile, :] for q in range(planes)]
                for p in range(planes):
                    total = partial[side * planes + p, pl.ds(8 * t, 8), :]
                    for j in range(1, REACH + 1):
                        q = p + j - planes if side == 1 else planes + p - j
                        if 0 <= q < planes:
                            total = total + weights[j] * window[q]
                    yield p, start + p, t, tile, total

        outer = (0, total_planes - planes)

        def begin(f):
            for i, p, _, t, _, _, total in apply(f, outer, (0, 1)):
                partial[i * planes + p, pl.ds(8 * t, 8), :] = total

        def await_halos(f, parity):
            for side in range(2):
                halo(f, side, parity).wait_send()
            for side in range(2):
                there = total_planes + planes if side == 1 else 0
                landed = f.at[pl.ds(there, planes), body, :]
                remote(
                    landed, landed, halo_send.at[side], halo_recv.at[side, parity], partner
                ).wait_recv()

        def step(m, c):
            now, then, before = (fields[(c + i) % 3] for i in range(3))
            gain = jnp.where(m == 1, 0.5, 1.0)

            def settle(plane, t, tile, total):
                following = gain * total - before[planes + plane, tile, :]
                put(then, planes + plane, t, following)
                return following

            begin(now)

            def inner(k, carry):
                start = planes + 2 * planes * k
                spans = (start, start + planes)
                for _, _, plane, t, tile, _, total in apply(now, spans, (None, None)):
                    settle(plane, t, tile, total)
                return carry

            lax.fori_loop(0, slabs // 2 - 1, inner, 0)
            parity = lax.rem(m - 1, 2)
            await_halos(now, parity)
            for side in range(2):
                for p, plane, t, tile, total in finish(now, outer[side], side):
                    hold(side, p, t, settle(plane, t, tile, total))
                halo(then, side, 1 - parity).start()

        def three(r, carry):
            for c in range(3):
                step(3 * r + c + 1, c)
            return carry

        lax.fori_loop(0, DEGREE // 3, three, 0)
        final = field_0

        flat_packed = packed.reshape(slabs, 2 * planes * CHUNKS, LANES)
        gather_rows = [lax.rem(3 * row + i, 8) for i in range(2)]
        lane6 = lax.broadcasted_iota(jnp.int32, (TILES, LANES), 1)

        def give(slot):
            return remote(
                packed.at[slot],
                out_ref.at[:, my_band],
                out_send.at[slot],
                out_recv.at[my_band],
                core * slabs + slot,
            )

        def give_here(slot):
            return pltpu.make_async_copy(
                packed.at[slot], out_ref.at[:, my_band], out_recv.at[my_band]
            )

        def pack(i, carry):
            slot = jnp.where(core == my_band, slabs - 1 - i, i + 1 - 2 * lax.rem(i, 2))

            for p in range(planes):
                plane = planes + slot * planes + p
                for part_index in range(2):
                    lot = 2 * p + part_index
                    for t in range(TILES):
                        v = final[plane, pl.ds(PAD + 8 * t, 8), :] * final_scale
                        v = jnp.take_along_axis(v, gather_rows[part_index], axis=0)
                        v = pltpu.roll(v, 0, 1, stride=16, stride_axis=0)
                        rolled[lot, pl.ds(8 * t, 8), :] = v
            for p in range(planes):
                for part_index in range(2):
                    lot = 2 * p + part_index
                    picks = [
                        rolled[lot, pl.ds((3 * i + 5 * part_index) % 8, TILES, stride=8), :]
                        for i in range(8)
                    ]

                    def choose(*ends):
                        start = ends[0]
                        v = picks[start + len(ends) - 1]
                        for i in range(len(ends) - 2, -1, -1):
                            v = jnp.where(lane6 < ends[i + 1], picks[start + i], v)
                        return v

                    rows = (choose(0, 48, 96), choose(2, 16, 64, 112), choose(5, 32, 80))
                    base = (part_index * planes + p) * CHUNKS
                    for j in range(PER_TILE):
                        flat_packed[slot, pl.ds(base + j, TILES, stride=PER_TILE), :] = rows[j]

            goal = core * slabs + slot
            aside = goal == lax.rem(me - core + 5, n) if relay_on else jnp.bool_(False)

            @pl.when((goal != me) & jnp.logical_not(aside))
            def _():
                give(slot).start()

            if relay_on:

                @pl.when(aside)
                def _():
                    remote(
                        packed.at[slot],
                        relay_out,
                        out_send.at[slot],
                        relay_recv.at[1],
                        lax.rem(me - core + n - 1, n),
                    ).start()

            @pl.when(core * slabs + slot == me)
            def _():
                give_here(slot).start()

            return carry

        lax.fori_loop(0, slabs, pack, 0)

        begin(final)

        def gather_up(sums, t, value, total):
            tops, bottoms = sums
            tops[t % 2] = tops[t % 2] + value * total
            bottoms[t % 2] = bottoms[t % 2] + value * value

        def inner_sums(k, carry):
            sums = list(carry[0]), list(carry[1])
            start = planes + 2 * planes * k
            for _, _, _, t, _, value, total in apply(
                final, (start, start + planes), (None, None)
            ):
                gather_up(sums, t, value, total)
            return tuple(sums[0]), tuple(sums[1])

        carry = ((zero, zero), (zero, zero))
        carry = lax.fori_loop(0, slabs // 2 - 1, inner_sums, carry)
        tops, bottoms = sums = list(carry[0]), list(carry[1])
        await_halos(final, DEGREE % 2)
        for side in range(2):
            for _, plane, t, tile, total in finish(final, outer[side], side):
                gather_up(sums, t, final[planes + plane, tile, :], total)
        top = jnp.sum(tops[0] + tops[1], keepdims=True)
        bottom = jnp.sum(bottoms[0] + bottoms[1], keepdims=True)
        left = lax.broadcasted_iota(jnp.int32, (1, LANES), 1) < LANES // 2
        part[my_place] = jnp.where(left, top, bottom)
        for d in range(1, n):
            remote(
                part.at[my_place],
                part.at[my_place],
                send_red.at[d],
                recv_red.at[my_place],
                lax.rem(me + d, n),
            ).start()

    for w in range(workers):

        @pl.when(me != worker(w // 2, w % 2))
        def _():
            remote(part.at[w], part.at[w], send_red.at[0], recv_red.at[w], partner).wait_recv()

    kweight, fermi = kweight_ref[0], fermi_ref[0]
    e_half, c_half = half_width[0:1, :], centre[0:1, :]
    term = jnp.zeros((1, LANES), jnp.float32)
    for b in range(BANDS):
        both = part[2 * b] + part[2 * b + 1]
        energy = (0.5 * e_half) * (both / pltpu.roll(both, LANES // 2, 1)) + c_half
        energy_ref[0, b] = energy[0, 0]
        term = term + energy / (1.0 + jnp.exp((energy - fermi) / smearing))
    part_k[kpt] = kweight * term

    def across(d, source, target):
        return pltpu.make_async_remote_copy(
            src_ref=part_k.at[source],
            dst_ref=part_k.at[source],
            send_sem=send_k.at[d],
            recv_sem=recv_k.at[source],
            device_id=(target, me),
            device_id_type=MESH,
        )

    for d in range(1, members_k):
        across(d, kpt, lax.rem(kpt + d, members_k)).start()
    for d in range(1, members_k):
        source = lax.rem(kpt + d, members_k)
        across(d, source, source).wait_recv()
    grand = jnp.zeros((1, LANES), jnp.float32)
    for k in range(members_k):
        grand = grand + part_k[k]
    total_ref[0, 0] = grand[0, 0]

    for b in range(BANDS):
        landing = out_ref.at[:, b]
        remote(landing, landing, out_send.at[0], out_recv.at[b], partner).wait_recv()

    for i in range(BANDS):
        wave, pot, target = deliver(i)

        @pl.when(target != me)
        def _():
            wave.wait_send()

        @pl.when((target != me) & gives_pot)
        def _():
            pot.wait_send()

    for d in range(1, members_k):
        across(d, kpt, lax.rem(kpt + d, members_k)).wait_send()

    @pl.when(is_worker)
    def _():
        for d in range(1, n):
            remote(
                part.at[my_place],
                part.at[my_place],
                send_red.at[d],
                recv_red.at[my_place],
                lax.rem(me + d, n),
            ).wait_send()

        def drain(slot, carry):
            @pl.when(core * slabs + slot != me)
            def _():
                remote(
                    packed.at[slot],
                    out_ref.at[:, my_band],
                    out_send.at[slot],
                    out_recv.at[my_band],
                    core * slabs + slot,
                ).wait_send()

            return carry

        lax.fori_loop(0, slabs, drain, 0)

        def drain_pot(slot, carry):
            @pl.when(lax.rem(slot, members_k) == kpt)
            def _():
                for d in range(1, members_k):
                    pass_pot(slot, d).wait_send()

            return carry

        lax.fori_loop(0, slabs, drain_pot, 0)


def per_device(bands, potential, table, kweight, lowest, cut, upper, fermi):
    n = lax.axis_size("grid")
    members_k = lax.axis_size("kpt")
    planes = bands.shape[3]
    pieces = 2 * planes
    flat = pieces * CHUNKS

    raw = bands[0].transpose(0, 2, 1, 3).reshape(pieces, BANDS, CHUNKS, LANES)
    raw = with_layout_constraint(raw, Layout((0, 2, 1, 3)))
    raw = raw.transpose(0, 2, 1, 3).reshape(flat, BANDS, 1, LANES)

    vmem, smem = pltpu.VMEM, pltpu.SMEM
    anywhere = pl.BlockSpec(memory_space=pl.ANY)
    hbm = pl.BlockSpec(memory_space=pltpu.HBM)
    scalar = pl.BlockSpec(memory_space=smem)
    slabs = n // 2
    workers = 2 * BANDS
    total_planes = slabs * planes
    dma = pltpu.SemaphoreType.DMA
    f32 = jnp.float32
    out, energy, total = pl.pallas_call(
        functools.partial(kernel, n, members_k, planes),
        name="cheb",
        out_shape=(
            jax.ShapeDtypeStruct((flat, BANDS, 1, LANES), f32),
            jax.ShapeDtypeStruct((1, BANDS), f32),
            jax.ShapeDtypeStruct((1, 1), f32),
        ),
        in_specs=[scalar] + [hbm] * 7,
        out_specs=(hbm, scalar, scalar),
        scratch_shapes=[
            smem((1,), f32),
            smem((1,), f32),
            smem((1,), f32),
            smem((1,), f32),
            smem((1,), f32),
            vmem((BANDS, flat, 1, LANES), f32),
            vmem((planes, SIDE * SIDE), f32),
            vmem((total_planes + 2 * planes, ROWS, LANES), f32),
            vmem((total_planes + 2 * planes, ROWS, LANES), f32),
            vmem((total_planes + 2 * planes, ROWS, LANES), f32),
            vmem((2 * LANES, 2 * LANES), jnp.bfloat16),
            vmem((LANES, LANES), f32),
            vmem((total_planes, SIDE, LANES), f32),
            vmem((slabs, flat, 1, LANES), f32),
            vmem((slabs, planes, SIDE * SIDE), f32),
            vmem((2, planes, SIDE, LANES), f32),
            vmem((2 * planes, SIDE, LANES), f32),
            vmem((2 * planes, SIDE, LANES), f32),
            vmem((slabs, flat, 1, LANES), f32),
            vmem((workers, 1, LANES), f32),
            vmem((members_k, 1, LANES), f32),
            vmem((flat, 1, LANES), f32),
            vmem((flat, 1, LANES), f32),
            dma((8,)),
            dma((BANDS,)),
            dma((slabs,)),
            dma((BANDS,)),
            dma((slabs,)),
            dma((slabs, members_k)),
            dma((2,)),
            dma((2, 2)),
            dma((slabs,)),
            dma((BANDS,)),
            dma((n,)),
            dma((workers,)),
            dma((members_k,)),
            dma((members_k,)),
            dma((2,)),
            dma((2,)),
        ],
        compiler_params=pltpu.CompilerParams(
            collective_id=0, has_side_effects=True, vmem_limit_bytes=62 * 1024 * 1024
        ),
    )(table, kweight, lowest, cut, upper, fermi, raw, potential)
    filtered = out.reshape(pieces, CHUNKS, BANDS, LANES).transpose(0, 2, 1, 3)
    filtered = filtered.reshape(2, planes, BANDS, SIDE * SIDE).transpose(0, 2, 1, 3)[None]
    return filtered, energy, total[0]


def solution(mesh):
    in_specs = (
        P("kpt", None, None, "grid", None),
        P("grid", None),
        P("kpt", None),
        P("kpt"),
        P("kpt"),
        P("kpt"),
        P("kpt"),
        P(),
    )
    out_specs = (P("kpt", None, None, "grid", None), P("kpt", None), P())
    return jax.shard_map(
        per_device, mesh=mesh, in_specs=in_specs, out_specs=out_specs, check_vma=False
    )
```
